32 devices in a mesh: groups: 1, ctx: 8 (over z, y), head: 2 (over x), rep: 2 (over core).
Axes of the slice: x: 2, y: 2, z: 4, core: 2. Of those that a mesh axis runs over, the one named last changes fastest.
Arguments:
- queries: bfloat16 [16, 512, 4096], P(('groups', 'ctx'), 'rep', 'head'), may hold values from -6 to 6
- prefill_keys: bfloat16 [16, 512, 1024], P(('groups', 'ctx'), 'rep', 'head'), may hold values from -6 to 6
- prefill_values: bfloat16 [16, 512, 1024], P(('groups', 'ctx'), 'rep', 'head'), may hold values from -6 to 6
- context_keys: bfloat16 [16384, 1024], P(('groups', 'ctx'), 'head'), may hold values from -6 to 6
- context_values: bfloat16 [16384, 1024], P(('groups', 'ctx'), 'head'), may hold values from -6 to 6
- picks: int32 [16, 32, 3], P(('groups', 'ctx'), 'head'), may hold values from 0 to 47, as said below
Outputs:
- attended: bfloat16 [16, 512, 4096], P(('groups', 'ctx'), 'rep', 'head')
The draws below stay inside these ranges and needn't reach their ends.
Inputs may be any that keep to these rules, and one draw needn't show every extreme that they name: `picks`: row [b, h] is increasing; its last entry is 32 + b and its first two are cache blocks. Among the first two entries of the rows of the 2 query blocks that start at a multiple of 2 and the 16 heads of one run that starts at a multiple of 16, at most 16 lie in the 4 blocks that start at one multiple of 4, and for every such set of rows some such set of blocks holds exactly 16 of them.
All inputs are finite; a program needn't handle non-finite values.
Results may differ from the reference program's by a relative error of at most 0.0055.
Values may be sent and summed in bfloat16 or wider, within the bound.
A program may use at most 64 MiB of HBM per device.

```python
import jax
import jax.numpy as jnp
from jax import lax

QUERY_HEAD_COUNT = 32
KEY_VALUE_HEADS = 8
HEAD_WIDTH = 128
BLOCK_TOKENS = 512
QB_DEV = 2
BLK_DEV = 4
CACHE_BLOCKS = 32
CACHE_TOKENS = 16384
QUERY_BLOCKS = 16
PREFILL_TOKENS = 8192
CAP = 16
N_CTX = 8
N_HEAD = 2


def key_record_field(key, salt, stack_height):
    array_shape = (stack_height, KEY_VALUE_HEADS, HEAD_WIDTH)
    record_field = jnp.clip(jax.random.normal(jax.random.fold_in(key, salt), array_shape, jnp.float32), -6.0, 6.0)
    return record_field.reshape(stack_height, KEY_VALUE_HEADS * HEAD_WIDTH).astype(jnp.bfloat16)


def draw_queries(key, part):
    array_shape = (PREFILL_TOKENS, QUERY_HEAD_COUNT, HEAD_WIDTH)
    record_field = jnp.clip(jax.random.normal(jax.random.fold_in(key, 11), array_shape, jnp.float32), -6.0, 6.0)
    return record_field.reshape(QUERY_BLOCKS, BLOCK_TOKENS, QUERY_HEAD_COUNT * HEAD_WIDTH).astype(jnp.bfloat16)


def draw_prefill_keys(key, part):
    return key_record_field(key, 21, PREFILL_TOKENS).reshape(QUERY_BLOCKS, BLOCK_TOKENS, KEY_VALUE_HEADS * HEAD_WIDTH)


def draw_context_keys(key, part):
    return key_record_field(key, 31, CACHE_TOKENS)


def draw_picks(key, part):
    head_grouping = QUERY_HEAD_COUNT // N_HEAD
    runs = QB_DEV * head_grouping
    needed = 2 * runs
    slot_total = N_CTX * CAP
    tokens = jnp.arange(slot_total)
    columns = []
    for head_index in range(N_HEAD):
        head_key = jax.random.fold_in(key, 100 + head_index)
        hottest = jax.random.randint(jax.random.fold_in(head_key, 1), (), 0, N_CTX)

        def single(row_key, row_index):
            subkeys = jax.random.split(row_key, 5)
            shuffled = jax.random.permutation(subkeys[0], slot_total)
            ranking = jnp.where(tokens // CAP == hottest, tokens % CAP, CAP + shuffled)
            taken = jnp.argsort(ranking, stable=True)[:needed]
            taken = jax.random.permutation(subkeys[1], taken)
            holders = (taken // CAP).reshape(runs, 2)
            leading = jax.random.randint(subkeys[2], (runs,), 0, BLK_DEV)
            shifted = (leading + 1 + jax.random.randint(subkeys[3], (runs,), 0, BLK_DEV - 1)) % BLK_DEV
            loose = jax.random.randint(subkeys[4], (runs,), 0, BLK_DEV)
            trailing = jnp.where(holders[:, 0] == holders[:, 1], shifted, loose)
            earlier = holders[:, 0] * BLK_DEV + leading
            later = holders[:, 1] * BLK_DEV + trailing
            ownblock = CACHE_BLOCKS + row_index * QB_DEV + jnp.arange(runs, dtype=jnp.int32) // head_grouping
            stacked = jnp.stack([jnp.minimum(earlier, later), jnp.maximum(earlier, later), ownblock], axis=1)
            return stacked.reshape(QB_DEV, head_grouping, 3)
        row_keys = jax.random.split(jax.random.fold_in(head_key, 2), N_CTX)
        columns.append(jax.vmap(single)(row_keys, jnp.arange(N_CTX, dtype=jnp.int32)))
    return jnp.concatenate(columns, axis=2).reshape(QUERY_BLOCKS, QUERY_HEAD_COUNT, 3).astype(jnp.int32)


def block_levels(stream_key, extent, cuts, smallest, largest):
    factor_of, own = 1.0, jax.random.fold_in(stream_key, 6)
    for axis_at, blocks in cuts:
        heights = jnp.exp(jax.random.uniform(jax.random.fold_in(own, axis_at), (blocks,), jnp.float32, smallest / len(cuts), largest / len(cuts)))
        factor_of = factor_of * jnp.repeat(heights, extent[axis_at] // blocks).reshape([-1 if axis == axis_at else 1 for axis in range(len(extent))])
    return factor_of


def normal_values(key, extent, scale, most, shards=(), kind=jnp.bfloat16):
    array = scale * jax.random.normal(key, extent, jnp.float32)
    if shards:
        array = array * block_levels(key, extent, shards, -0.22, 0.18)
    return jnp.clip(array, -most, most).astype(kind)


def setup_inputs(seed: int = 0, part: int = 0) -> dict:
    arg_keys = jax.random.split(jax.random.key(seed), 7)
    part_splits = jax.random.split(jax.random.fold_in(arg_keys[6], part), 7)
    return {
        "queries": draw_queries(jax.random.fold_in(jax.random.fold_in(arg_keys[6], part), 71), part),
        "prefill_keys": draw_prefill_keys(jax.random.fold_in(jax.random.fold_in(arg_keys[6], part), 71), part),
        "prefill_values": normal_values(part_splits[2], (QUERY_BLOCKS, BLOCK_TOKENS, KEY_VALUE_HEADS * HEAD_WIDTH), 1.0, 6.0, ((0, 8), (1, 2), (2, 2))),
        "context_keys": draw_context_keys(jax.random.fold_in(jax.random.fold_in(arg_keys[6], part), 71), part),
        "context_values": normal_values(part_splits[4], (CACHE_TOKENS, KEY_VALUE_HEADS * HEAD_WIDTH), 1.0, 6.0, ((0, 8), (1, 2))),
        "picks": draw_picks(jax.random.fold_in(jax.random.fold_in(arg_keys[6], part), 71), part),
    }


NEGATIVE = -1e30


def partial_attention(scores, values, allowed, pattern):
    scores = jnp.where(allowed, scores, NEGATIVE)
    highest = jnp.max(scores, axis=-1, keepdims=True)
    weights = jnp.exp(scores - highest)
    totals = jnp.sum(weights, axis=-1, keepdims=True)
    rounded = lax.optimization_barrier(weights.astype(jnp.bfloat16)).astype(jnp.float32)
    mixed = jnp.einsum(pattern, rounded, values.astype(jnp.float32))
    return mixed / totals, highest[..., 0] + jnp.log(totals[..., 0])


def reference(queries, prefill_keys, prefill_values, context_keys, context_values, picks):
    head_grouping = QUERY_HEAD_COUNT // KEY_VALUE_HEADS
    scale = HEAD_WIDTH ** -0.5
    owning_head = jnp.arange(QUERY_HEAD_COUNT, dtype=jnp.int32) // head_grouping
    key_tiles = context_keys.reshape(CACHE_BLOCKS, BLOCK_TOKENS, KEY_VALUE_HEADS, HEAD_WIDTH)
    value_tiles = context_values.reshape(CACHE_BLOCKS, BLOCK_TOKENS, KEY_VALUE_HEADS, HEAD_WIDTH)
    places = jnp.arange(BLOCK_TOKENS, dtype=jnp.int32)
    causal = places[None, :] <= places[:, None]

    def one_block(block_index):
        block_queries = lax.dynamic_index_in_dim(queries, block_index, 0, keepdims=False).reshape(BLOCK_TOKENS, QUERY_HEAD_COUNT, HEAD_WIDTH).astype(jnp.float32)
        selected_block_keys = lax.dynamic_index_in_dim(prefill_keys, block_index, 0, keepdims=False).reshape(BLOCK_TOKENS, KEY_VALUE_HEADS, HEAD_WIDTH)[:, owning_head, :].astype(jnp.float32)
        selected_block_values = lax.dynamic_index_in_dim(prefill_values, block_index, 0, keepdims=False).reshape(BLOCK_TOKENS, KEY_VALUE_HEADS, HEAD_WIDTH)[:, owning_head, :].astype(jnp.float32)
        scores = jnp.einsum("rhd,jhd->hrj", block_queries, selected_block_keys) * scale
        own_mixed, own_log = partial_attention(scores, selected_block_values, causal, "hrj,jhd->hrd")
        chosen = lax.dynamic_index_in_dim(picks, block_index, 0, keepdims=False)
        parts = [own_mixed]
        logs = [own_log]
        for column in range(2):
            blocks = chosen[:, column]
            keys_here = key_tiles[blocks, :, owning_head, :].astype(jnp.float32)
            values_here = value_tiles[blocks, :, owning_head, :].astype(jnp.float32)
            scores = jnp.einsum("rhd,hjd->hrj", block_queries, keys_here) * scale
            mixed, logged = partial_attention(scores, values_here, True, "hrj,hjd->hrd")
            mixed = lax.optimization_barrier(mixed.astype(jnp.bfloat16)).astype(jnp.float32)
            parts.append(mixed)
            logs.append(logged)
        all_logs = jnp.stack(logs, 0)
        all_mixed = jnp.stack(parts, 0)
        peak = jnp.max(all_logs, axis=0, keepdims=True)
        shares = jnp.exp(all_logs - peak)
        merged = jnp.sum(shares[..., None] * all_mixed, axis=0) / jnp.sum(shares, axis=0)[..., None]
        return jnp.transpose(merged, (1, 0, 2)).reshape(BLOCK_TOKENS, QUERY_HEAD_COUNT * HEAD_WIDTH).astype(jnp.bfloat16)

    return lax.map(one_block, jnp.arange(QUERY_BLOCKS, dtype=jnp.int32))
```

```python
import functools
import math

import jax
import jax.numpy as jnp
import numpy as np
from jax import lax
from jax.experimental import pallas as pl
from jax.experimental.pallas import tpu as pltpu
from jax.sharding import PartitionSpec as P


HEAD_WIDTH = 128
BLOCK_TOKENS = 512


NEGATIVE = -1e30


def from_behind(value, axis, steps):
    count = lax.axis_size(axis)
    first, last = (max(0, -steps), min(count, count - steps))
    return lax.ppermute(value, axis, [(source, source + steps) for source in range(first, last)])


def partial_attention(scores, values, allowed, pattern):
    scores = jnp.where(allowed, scores, NEGATIVE)
    highest = jnp.max(scores, axis=-1, keepdims=True)
    weights = jnp.exp(scores - highest)
    totals = jnp.sum(weights, axis=-1, keepdims=True)
    mixed = jnp.einsum(
        pattern, weights.astype(jnp.bfloat16), values, preferred_element_type=jnp.float32
    )
    return (mixed / totals, highest[..., 0] + jnp.log(totals[..., 0]))


def assign_slots(chosen, blocks_here, capacity):
    flat = chosen.reshape(-1)
    holders = flat // blocks_here
    places = jnp.arange(flat.shape[0])
    earlier = jnp.sum(
        (holders[:, None] == holders[None, :]) & (places[None, :] < places[:, None]), axis=1
    )
    return (holders * capacity + earlier, flat - holders * blocks_here)


def routed_body(queries, prefill_keys, prefill_values, context_keys, context_values, picks):
    local_count = queries.shape[0]
    stack_height = queries.shape[1]
    query_heads = queries.shape[2] // HEAD_WIDTH
    key_heads = prefill_keys.shape[2] // HEAD_WIDTH
    head_grouping = query_heads // key_heads
    blocks_here = context_keys.shape[0] // BLOCK_TOKENS
    ctx_size = lax.axis_size("ctx")
    pick_count = 2 * local_count * query_heads
    capacity = max(2, 2 * pick_count // ctx_size)
    slot_count = ctx_size * capacity
    scale = HEAD_WIDTH ** (-0.5)
    rep_index = lax.axis_index("rep")
    earlier_keys, earlier_values = from_behind((prefill_keys, prefill_values), "rep", 1)
    selected_block_keys = jnp.concatenate([earlier_keys, prefill_keys], 1).reshape(
        local_count, 2 * stack_height, key_heads, HEAD_WIDTH
    )
    selected_block_values = jnp.concatenate([earlier_values, prefill_values], 1).reshape(
        local_count, 2 * stack_height, key_heads, HEAD_WIDTH
    )
    grouped = queries.reshape(local_count, stack_height, key_heads, head_grouping, HEAD_WIDTH)
    query_place = rep_index * stack_height + jnp.arange(stack_height)
    key_place = (rep_index - 1) * stack_height + jnp.arange(2 * stack_height)
    allowed = (key_place[None, :] <= query_place[:, None]) & (key_place[None, :] >= 0)

    def own_block(paired):
        rows_here, keys_here, values_here = paired
        scores = (
            jnp.einsum("rkgd,jkd->kgrj", rows_here, keys_here, preferred_element_type=jnp.float32)
            * scale
        )
        return partial_attention(scores, values_here, allowed, "kgrj,jkd->kgrd")

    own_mixed, own_log = lax.map(own_block, (grouped, selected_block_keys, selected_block_values))
    own_mixed = own_mixed.reshape(local_count, query_heads, stack_height, HEAD_WIDTH)
    own_log = own_log.reshape(local_count, query_heads, stack_height)
    targets, local_blocks = assign_slots(picks[:, :, :2], blocks_here, capacity)
    routing = targets[:, None] == jnp.arange(slot_count)[None, :]
    sending = routing.astype(jnp.bfloat16).reshape(local_count, query_heads, 2, slot_count)
    by_head = queries.reshape(local_count, stack_height, query_heads, HEAD_WIDTH)
    outbound = jnp.einsum("qhps,qrhd->srd", sending, by_head, preferred_element_type=jnp.float32)
    outbound = outbound.astype(jnp.bfloat16).reshape(ctx_size, capacity, stack_height, HEAD_WIDTH)
    pick_heads = jnp.arange(pick_count) // 2 % query_heads // head_grouping
    key_tiles = context_keys.reshape(blocks_here, BLOCK_TOKENS, key_heads, HEAD_WIDTH)
    value_tiles = context_values.reshape(blocks_here, BLOCK_TOKENS, key_heads, HEAD_WIDTH)
    block_label = jnp.sum(jnp.where(routing, local_blocks[:, None], 0), axis=0)
    head_label = jnp.sum(jnp.where(routing, pick_heads[:, None], 0), axis=0)
    labels = jnp.stack([block_label, head_label], axis=-1).reshape(ctx_size, capacity, 2)
    inbound = lax.all_to_all(outbound, "ctx", split_axis=0, concat_axis=0, tiled=True)
    arrived = lax.all_to_all(labels, "ctx", split_axis=0, concat_axis=0, tiled=True)
    leading = inbound.shape[:2]

    def single(paired):
        rows_in, position = paired
        anchor = (position[0], 0, position[1], 0)
        keys_tile = lax.dynamic_slice(key_tiles, anchor, (1, BLOCK_TOKENS, 1, HEAD_WIDTH)).reshape(
            BLOCK_TOKENS, HEAD_WIDTH
        )
        values_tile = lax.dynamic_slice(
            value_tiles, anchor, (1, BLOCK_TOKENS, 1, HEAD_WIDTH)
        ).reshape(BLOCK_TOKENS, HEAD_WIDTH)
        scores = (
            lax.dot_general(
                rows_in, keys_tile, (((1,), (1,)), ((), ())), preferred_element_type=jnp.float32
            )
            * scale
        )
        mixed, logged = partial_attention(scores, values_tile, True, "rj,jd->rd")
        return (mixed.astype(jnp.bfloat16), logged)

    flat_rows = inbound.reshape((-1,) + inbound.shape[2:])
    flat_labels = arrived.reshape(-1, 2)
    mixed, logged = lax.map(single, (flat_rows, flat_labels), batch_size=8)
    served = mixed.reshape(leading + mixed.shape[1:])
    served_logs = logged.reshape(leading + logged.shape[1:])
    answers = lax.all_to_all(served, "ctx", split_axis=0, concat_axis=0, tiled=True)
    answer_logs = lax.all_to_all(served_logs, "ctx", split_axis=0, concat_axis=0, tiled=True)
    gathered = answers.reshape(slot_count, stack_height, HEAD_WIDTH)[targets]
    gathered_logs = answer_logs.reshape(slot_count, stack_height)[targets]
    remote_mixed = gathered.astype(jnp.float32).reshape(
        local_count, query_heads, 2, stack_height, HEAD_WIDTH
    )
    remote_logs = gathered_logs.reshape(local_count, query_heads, 2, stack_height)
    all_logs = jnp.concatenate([own_log[:, :, None], remote_logs], axis=2)
    all_mixed = jnp.concatenate([own_mixed[:, :, None], remote_mixed], axis=2)
    peak = jnp.max(all_logs, axis=2, keepdims=True)
    shares = jnp.exp(all_logs - peak)
    merged = jnp.sum(shares[..., None] * all_mixed, axis=2) / jnp.sum(shares, axis=2)[..., None]
    return (
        jnp.transpose(merged, (0, 2, 1, 3))
        .reshape(local_count, stack_height, query_heads * HEAD_WIDTH)
        .astype(jnp.bfloat16)
    )


RATE = HEAD_WIDTH ** (-0.5) * math.log2(math.e)
GATHER_LIMIT = 40 * 2**20


def fold(scores, values, peak, total, mixed):
    higher = jnp.maximum(peak, jnp.max(scores, axis=-1, keepdims=True))
    weights = jnp.exp2((scores - higher) * RATE)
    fade = jnp.exp2((peak - higher) * RATE)
    total = total * fade + jnp.sum(weights, axis=-1, keepdims=True)
    mixed = mixed * fade + jnp.dot(
        weights.astype(jnp.bfloat16), values, preferred_element_type=jnp.float32
    )
    return higher, total, mixed


def score(rows, keys):
    return lax.dot_general(
        rows, keys, (((1,), (1,)), ((), ())), preferred_element_type=jnp.float32
    )


def pack(peak, total):
    lane = lax.broadcasted_iota(jnp.int32, (peak.shape[0], HEAD_WIDTH), 1)
    return jnp.where(lane < HEAD_WIDTH // 2, peak, total)


def unpack(packed):
    return packed[:, :1], packed[:, HEAD_WIDTH // 2 : HEAD_WIDTH // 2 + 1]


def own_kernel(grouping, late_ref, q_ref, ek_ref, ev_ref, k_ref, v_ref, mixed_ref, stat_ref):
    height = q_ref.shape[1]

    def unit(index, carry):
        block = index // grouping
        lanes = pl.ds(pl.multiple_of(index % grouping * HEAD_WIDTH, HEAD_WIDTH), HEAD_WIDTH)
        rows = q_ref[block, :, lanes]
        scores = score(rows, k_ref[block])
        row = lax.broadcasted_iota(jnp.int32, scores.shape, 0)
        column = lax.broadcasted_iota(jnp.int32, scores.shape, 1)
        scores = jnp.where(column <= row, scores, NEGATIVE)
        peak = jnp.full((height, 1), NEGATIVE, jnp.float32)
        total = jnp.zeros((height, 1), jnp.float32)
        mixed = jnp.zeros((height, HEAD_WIDTH), jnp.float32)
        peak, total, mixed = fold(scores, v_ref[block], peak, total, mixed)
        mixed_ref[index] = mixed
        stat_ref[index] = pack(peak, total)

        @pl.when(late_ref[0] > 0)
        def _():
            peak, total = unpack(stat_ref[index])
            peak, total, mixed = fold(
                score(rows, ek_ref[block]), ev_ref[block], peak, total, mixed_ref[index]
            )
            mixed_ref[index] = mixed
            stat_ref[index] = pack(peak, total)

        return carry

    lax.fori_loop(0, q_ref.shape[0] * grouping, unit, 0)


def pick_kernel(grouping, pieces, per_piece, last, table_ref, q_ref, *refs):
    keys, values = refs[:pieces], refs[pieces : 2 * pieces]
    mixed_in, stat_in = refs[2 * pieces : 2 * pieces + 2]
    mixed_ref, stat_ref = refs[-2:]
    count = q_ref.shape[0] * grouping
    group = pl.program_id(0)
    mixed_ref[...] = mixed_in[...]
    stat_ref[...] = stat_in[...]

    def unit(place, carry):
        index = place // 2
        block = index // grouping
        code = table_ref[group * count * 2 + place]
        for piece in range(pieces):

            @pl.when((code >= piece * per_piece) & (code < (piece + 1) * per_piece))
            def _():
                lanes = pl.ds(pl.multiple_of(index % grouping * HEAD_WIDTH, HEAD_WIDTH), HEAD_WIDTH)
                rows = q_ref[block, :, lanes]
                tile = pl.ds(
                    pl.multiple_of((code - piece * per_piece) * BLOCK_TOKENS, BLOCK_TOKENS),
                    BLOCK_TOKENS,
                )
                peak, total = unpack(stat_ref[index])
                peak, total, mixed = fold(
                    score(rows, keys[piece][tile, :]),
                    values[piece][tile, :],
                    peak,
                    total,
                    mixed_ref[index],
                )
                mixed_ref[index] = mixed
                stat_ref[index] = pack(peak, total)

        return carry

    lax.fori_loop(0, count * 2, unit, 0)
    if last:
        out_ref = refs[-3]
        for index in range(count):
            _, total = unpack(stat_ref[index])
            at = index % grouping * HEAD_WIDTH
            out_ref[index // grouping, :, at : at + HEAD_WIDTH] = (
                mixed_ref[index] / total
            ).astype(out_ref.dtype)


def cost(units, height, moved):
    each = height * BLOCK_TOKENS
    return pl.CostEstimate(
        flops=units * each * 4 * HEAD_WIDTH, transcendentals=units * each, bytes_accessed=moved
    )


def own_call(queries, earlier_keys, earlier_values, keys, values, late):
    blocks, height, width = queries.shape
    key_heads = keys.shape[2] // HEAD_WIDTH
    grouping = width // keys.shape[2]
    count = blocks * grouping
    q_spec = pl.BlockSpec((blocks, height, grouping * HEAD_WIDTH), lambda g, *_: (0, 0, g))
    k_spec = pl.BlockSpec((blocks, height, HEAD_WIDTH), lambda g, *_: (0, 0, g))
    s_spec = pl.BlockSpec((None, count, height, HEAD_WIDTH), lambda g, *_: (g, 0, 0, 0))
    state = jax.ShapeDtypeStruct((key_heads, count, height, HEAD_WIDTH), jnp.float32)
    return pl.pallas_call(
        functools.partial(own_kernel, grouping),
        grid_spec=pltpu.PrefetchScalarGridSpec(
            num_scalar_prefetch=1,
            grid=(key_heads,),
            in_specs=[q_spec] + [k_spec] * 4,
            out_specs=[s_spec] * 2,
        ),
        out_shape=[state, state],
        cost_estimate=cost(key_heads * count, height, 12 * 2**20),
        name="own_attend",
    )(late, queries, earlier_keys, earlier_values, keys, values)


def pick_call(queries, keys, values, table, state, last):
    blocks, height, width = queries.shape
    key_heads = keys[0].shape[1] // HEAD_WIDTH
    grouping = width // keys[0].shape[1]
    count = blocks * grouping
    rows = keys[0].shape[0]
    pieces = len(keys)
    q_spec = pl.BlockSpec((blocks, height, grouping * HEAD_WIDTH), lambda g, *_: (0, 0, g))
    k_spec = pl.BlockSpec((rows, HEAD_WIDTH), lambda g, *_: (0, g))
    s_spec = pl.BlockSpec((None, count, height, HEAD_WIDTH), lambda g, *_: (g, 0, 0, 0))
    shape = jax.ShapeDtypeStruct((key_heads, count, height, HEAD_WIDTH), jnp.float32)
    scratch = [pltpu.VMEM((count, height, HEAD_WIDTH), jnp.float32)] * 2
    return pl.pallas_call(
        functools.partial(pick_kernel, grouping, pieces, rows // BLOCK_TOKENS, last),
        grid_spec=pltpu.PrefetchScalarGridSpec(
            num_scalar_prefetch=1,
            grid=(key_heads,),
            in_specs=[q_spec] + [k_spec] * (2 * pieces) + [s_spec] * 2,
            out_specs=q_spec if last else [s_spec] * 2,
            scratch_shapes=scratch if last else [],
        ),
        out_shape=jax.ShapeDtypeStruct(queries.shape, queries.dtype) if last else [shape, shape],
        input_output_aliases={} if last else {2 + 2 * pieces: 0, 3 + 2 * pieces: 1},
        cost_estimate=cost(key_heads * count // 2, height, 24 * 2**20),
        name="pick_attend",
    )(table, queries, *keys, *values, *state)


def gathered_body(queries, prefill_keys, prefill_values, context_keys, context_values, picks):
    key_heads = prefill_keys.shape[2] // HEAD_WIDTH
    local_count, query_heads = picks.shape[:2]
    grouping = query_heads // key_heads
    blocks_here = context_keys.shape[0] // BLOCK_TOKENS
    half = blocks_here // 2
    size = lax.axis_size("ctx")
    cycle = list(range(0, size, 2)) + list(range(1, size, 2))[::-1]
    spot = {member: at for at, member in enumerate(cycle)}
    me = lax.axis_index("ctx")
    rep = lax.axis_index("rep")
    forward = [(cycle[i], cycle[(i + 1) % size]) for i in range(size)]
    backward = [(b, a) for a, b in forward]

    def origin(steps):
        return jnp.asarray(
            np.array([cycle[(spot[c] - steps) % size] for c in range(size)], np.int32)
        )[me]

    def swap(value):
        return lax.ppermute(value, "rep", [(0, 1), (1, 0)])

    chosen = picks[:, :, :2].reshape(local_count, key_heads, grouping, 2)
    chosen = jnp.transpose(chosen, (1, 0, 2, 3)).reshape(-1)
    holder, within = chosen // blocks_here, chosen % blocks_here
    crossed = (within // half != rep).astype(jnp.int32)
    code = crossed * half + within % half

    mine = tuple(
        lax.dynamic_slice_in_dim(x, rep * half * BLOCK_TOKENS, half * BLOCK_TOKENS, 0)
        for x in (context_keys, context_values)
    )
    up, down = mine, mine
    up = tuple(lax.ppermute(x, "ctx", forward) for x in up)
    down = tuple(lax.ppermute(x, "ctx", backward) for x in down)
    earlier_keys, earlier_values = from_behind((prefill_keys, prefill_values), "rep", 1)
    state = own_call(
        queries, earlier_keys, earlier_values, prefill_keys, prefill_values, rep.reshape(1)
    )
    state = pick_call(
        queries,
        [context_keys],
        [context_values],
        jnp.where(holder == me, within, -1),
        state,
        False,
    )
    for step in range(1, size // 2):
        arrived = (up, down)
        if step < size // 2 - 1:
            up = tuple(lax.ppermute(x, "ctx", forward) for x in up)
            down = tuple(lax.ppermute(x, "ctx", backward) for x in down)
        else:
            final = (
                lax.ppermute(up[0], "ctx", forward),
                lax.ppermute(down[1], "ctx", backward),
            )
        pairs = [pair for got in arrived for pair in (got, tuple(swap(x) for x in got))]
        table = jnp.where(
            holder == origin(step),
            code,
            jnp.where(holder == origin(-step), 2 * half + code, -1),
        )
        state = pick_call(
            queries, [p[0] for p in pairs], [p[1] for p in pairs], table, state, False
        )
    other = tuple(swap(x) for x in final)
    table = jnp.where(holder == origin(size // 2), code, -1)
    return pick_call(queries, [final[0], other[0]], [final[1], other[1]], table, state, True)


def body(*args):
    keys = args[3]
    size = lax.axis_size("ctx")
    gathered = 2 * size * keys.size * keys.dtype.itemsize
    even = size % 2 == 0 and size >= 4 and keys.shape[0] // BLOCK_TOKENS % 2 == 0
    if even and lax.axis_size("rep") == 2 and gathered <= GATHER_LIMIT:
        return gathered_body(*args)
    return routed_body(*args)


def solution(mesh):
    return jax.shard_map(
        body,
        mesh=mesh,
        in_specs=(
            P(("groups", "ctx"), "rep", "head"),
            P(("groups", "ctx"), "rep", "head"),
            P(("groups", "ctx"), "rep", "head"),
            P(("groups", "ctx"), "head"),
            P(("groups", "ctx"), "head"),
            P(("groups", "ctx"), "head", None),
        ),
        out_specs=P(("groups", "ctx"), "rep", "head"),
        check_vma=False,
    )
```
